32 devices in a mesh: row: 8 (over z, core), col: 4 (over y, x).
Axes of the slice: x: 2, y: 2, z: 4, core: 2. Of those that a mesh axis runs over, the one named last changes fastest.
Arguments:
- design: float32 [4096, 65536], P('row', 'col'), may hold values from -0.0625 to 0.0625
- targets: float32 [32, 4096], P(None, 'row'), may hold values from -6 to 6
- warm_solution: float32 [32, 65536], P(None, ('col', 'row')), may hold values from -2 to 2
- warm_sparse: float32 [32, 65536], P(None, ('col', 'row')), may hold values from -2 to 2
- warm_dual: float32 [32, 65536], P(None, ('col', 'row')), may hold values from -1.5 to 1.5
- sparsity: float32 [32], replicated, may hold values from 0.02 to 0.2
Outputs:
- solution: float32 [32, 65536], P(None, ('col', 'row'))
- sparse: float32 [32, 65536], P(None, ('col', 'row'))
- scaled_dual: float32 [32, 65536], P(None, ('col', 'row'))
The draws below stay inside these ranges and needn't reach their ends.
All inputs are finite; a program needn't handle non-finite values.
Results may differ from the reference program's by a relative error of at most 0.0003.
Values sent between devices are 32-bit elements; how exact they have to be, the bound alone decides.
A program may use at most 128 MiB of HBM per device.

```python
import math
import jax
import jax.numpy as jnp
from jax import lax

N = 65536
K = 32
OUTER = 1
STEPS = 3
M = 4096


def strengthened(array, rng, source, target, shards_of, factor):
    owner, partner = [(jnp.arange(array.shape[position]) // (array.shape[position] // shards_of)).reshape([-1 if axis == position else 1 for axis in range(array.ndim)]) for position in (source, target)]
    chosen = jax.random.permutation(rng, shards_of)[partner]
    strong = (owner == chosen) | (owner == (partner + shards_of // 2) % shards_of)
    return jnp.where(strong, factor * array, array)


def block_scale(own_key, shape, pieces, least, top_value):
    def one(axis_at, shards_of):
        draws = jax.random.uniform(jax.random.fold_in(jax.random.fold_in(own_key, 6), axis_at), (shards_of,), jnp.float32, least / len(pieces), top_value / len(pieces))
        return jnp.repeat(jnp.exp(draws), shape[axis_at] // shards_of).reshape((-1,) + (1,) * (len(shape) - axis_at - 1))

    level = one(*pieces[0])
    for cut in pieces[1:]:
        level = level * one(*cut)
    return level


def bell_draw(stream_key, dims, deviation, limit, shards=(), dtype=jnp.bfloat16):
    array = jax.random.normal(stream_key, dims, jnp.float32) * deviation
    if len(shards) > 0:
        array = block_scale(stream_key, dims, shards, -0.22, 0.18) * array
    return jnp.clip(array, min=-limit, max=limit).astype(dtype)


def heavy_noise(stream_key, dims, spread, limit, split, heavy, dtype=jnp.bfloat16):
    values = spread * jax.random.normal(stream_key, dims, jnp.float32)
    if split:
        values = values * block_scale(stream_key, dims, split, -0.22, 0.18)
    return jnp.clip(strengthened(values, jax.random.fold_in(stream_key, 3), *heavy), -limit, limit).astype(dtype)


def setup_inputs(seed: int = 0) -> dict:
    key_list = jax.random.split(jax.random.key(seed), 7)
    design = heavy_noise(key_list[0], (M, N), (N // 4) ** -0.5, 0.0625, ((0, 8), (1, 4)), (0, 1, 8, 2.0), jnp.float32)
    targets = bell_draw(key_list[1], (K, M), 1.0, 6.0, ((1, 8),), jnp.float32)
    warm_solution = bell_draw(key_list[2], (K, N), 0.3, 2.0, ((1, 32),), jnp.float32)
    warm_sparse = bell_draw(key_list[3], (K, N), 0.3, 2.0, ((1, 32),), jnp.float32)
    warm_dual = bell_draw(key_list[4], (K, N), 0.2, 1.5, ((1, 32),), jnp.float32)
    sparsity = jnp.clip(jnp.exp(jax.random.uniform(key_list[5], (K,), jnp.float32, math.log(0.02), math.log(0.2))), 0.02, 0.2)
    return dict(design=design, targets=targets, warm_solution=warm_solution, warm_sparse=warm_sparse, warm_dual=warm_dual, sparsity=sparsity)


penalty = 0.5


def gram(design, vector):
    forward = lax.dot_general(vector, design, (((1,), (1,)), ((), ())), precision=lax.Precision.HIGHEST, preferred_element_type=jnp.float32)
    back = jnp.dot(forward, design, precision=lax.Precision.HIGHEST, preferred_element_type=jnp.float32)
    return back + penalty * vector


def reference(design, targets, warm_solution, warm_sparse, warm_dual, sparsity):
    fitted = jnp.dot(targets, design, precision=lax.Precision.HIGHEST, preferred_element_type=jnp.float32)
    thresh = (sparsity / penalty)[:, None]
    solution, sparse, scaled_dual = warm_solution, warm_sparse, warm_dual
    for outer in range(OUTER):
        rhs = fitted + penalty * (sparse - scaled_dual)
        residual = rhs - gram(design, solution)
        direction = residual
        norm_now = jnp.sum(residual * residual, axis=1, keepdims=True)
        for step in range(STEPS):
            image = gram(design, direction)
            alpha = norm_now / jnp.sum(direction * image, axis=1, keepdims=True)
            solution = solution + alpha * direction
            residual = residual - alpha * image
            norm_next = jnp.sum(residual * residual, axis=1, keepdims=True)
            direction = residual + (norm_next / norm_now) * direction
            norm_now = norm_next
        merged = solution + scaled_dual
        sparse = jnp.sign(merged) * jnp.maximum(jnp.abs(merged) - thresh, 0.0)
        scaled_dual = merged - sparse
    return solution, sparse, scaled_dual
```

```python
import functools

import jax
import jax.numpy as jnp
from jax import lax
from jax.experimental import pallas as pl
from jax.experimental.pallas import tpu as pltpu
from jax.sharding import PartitionSpec as P

STEPS = 3
LANES = 128
MESH = pl.DeviceIdType.MESH

penalty = 0.5


def halves(values):
    high = lax.reduce_precision(values, 8, 7)
    return high.astype(jnp.bfloat16), (values - high).astype(jnp.bfloat16)


def product(values, high, low, dims):
    rows = values.shape[0]
    top, rest = halves(values)
    dot = functools.partial(
        lax.dot_general, dimension_numbers=(dims, ((), ())), preferred_element_type=jnp.float32
    )
    both = dot(jnp.concatenate([top, rest], axis=0), high)
    return both[:rows] + (both[rows:] + dot(top, low))


def row_sums(values):
    return jnp.sum(values, axis=1, keepdims=True)


def exchange_kernel(
    nr, nc, part_ref, out_ref, total_ref, land, stat, stat_land, col_send, col_recv, row_send, row_recv
):
    row, col = lax.axis_index("row"), lax.axis_index("col")
    width = out_ref.shape[1]

    barrier = pltpu.get_barrier_semaphore()
    for s in range(1, nc):
        pl.semaphore_signal(
            barrier, inc=1, device_id={"col": lax.rem(col + s, nc)}, device_id_type=MESH
        )
    for s in range(1, nr):
        pl.semaphore_signal(
            barrier, inc=1, device_id={"row": lax.rem(row + s, nr)}, device_id_type=MESH
        )
    pl.semaphore_wait(barrier, nc + nr - 2)

    copies = []
    for s in range(1, nc):
        copy = pltpu.make_async_remote_copy(
            src_ref=part_ref,
            dst_ref=land.at[col],
            send_sem=col_send.at[s - 1],
            recv_sem=col_recv.at[s - 1],
            device_id={"col": lax.rem(col + s, nc)},
            device_id_type=MESH,
        )
        copy.start()
        copies.append(copy)
    land[col] = part_ref[...]
    for copy in copies:
        copy.wait_recv()
    summed = land[0]
    for s in range(1, nc):
        summed = summed + land[s]
    values = summed[:, :width]
    out_ref[...] = values
    square = jnp.sum(values * values, axis=1, keepdims=True)
    lane = lax.broadcasted_iota(jnp.int32, stat.shape, 1)
    mine = jnp.where(lane < LANES // 2, summed[:, width:], square)
    stat[...] = mine
    stat_land[row] = mine
    for s in range(1, nr):
        copy = pltpu.make_async_remote_copy(
            src_ref=stat,
            dst_ref=stat_land.at[row],
            send_sem=row_send.at[s - 1],
            recv_sem=row_recv.at[s - 1],
            device_id={"row": lax.rem(row + s, nr)},
            device_id_type=MESH,
        )
        copy.start()
        copies.append(copy)
    for copy in copies[nc - 1:]:
        copy.wait_recv()
    total = stat_land[0]
    for s in range(1, nr):
        total = total + stat_land[s]
    total_ref[...] = total
    for copy in copies:
        copy.wait_send()


def solution(mesh):
    nr, nc = mesh.shape["row"], mesh.shape["col"]

    def exchange(part, stats):
        rows, width = part.shape
        part = jnp.concatenate([part, jnp.broadcast_to(stats, (rows, LANES))], axis=1)
        vmem = pl.BlockSpec(memory_space=pltpu.VMEM)
        values, total = pl.pallas_call(
            functools.partial(exchange_kernel, nr, nc),
            out_shape=(
                jax.ShapeDtypeStruct((rows, width), jnp.float32),
                jax.ShapeDtypeStruct((rows, LANES), jnp.float32),
            ),
            in_specs=[vmem],
            out_specs=(vmem, vmem),
            scratch_shapes=[
                pltpu.VMEM((nc, rows, width + LANES), jnp.float32),
                pltpu.VMEM((rows, LANES), jnp.float32),
                pltpu.VMEM((nr, rows, LANES), jnp.float32),
                pltpu.SemaphoreType.DMA((nc - 1,)),
                pltpu.SemaphoreType.DMA((nc - 1,)),
                pltpu.SemaphoreType.DMA((nr - 1,)),
                pltpu.SemaphoreType.DMA((nr - 1,)),
            ],
            compiler_params=pltpu.CompilerParams(
                collective_id=0, has_side_effects=True, vmem_limit_bytes=8 * 1024 * 1024
            ),
        )(part)
        return values, total[:, :1], total[:, LANES - 1:]

    def on_device(design, targets, warm_solution, warm_sparse, warm_dual, sparsity):
        high, low = halves(design)

        def spread(vector):
            whole = lax.all_gather(vector, "row", axis=1, tiled=True)
            part = product(whole, high, low, ((1,), (1,)))
            return exchange(part, row_sums(vector * vector))

        def collect(values):
            part = product(values, high, low, ((1,), (0,)))
            return lax.psum_scatter(part, "row", scatter_dimension=1, tiled=True)

        solution, sparse, scaled_dual = warm_solution, warm_sparse, warm_dual
        thresh = (sparsity / penalty)[:, None]
        seen, _, _ = spread(solution)
        residual = collect(targets - seen) + penalty * ((sparse - scaled_dual) - solution)
        direction = along = norm_now = alpha = None
        for step in range(STEPS):
            seen, norm_next, square = spread(residual)
            energy = square + penalty * norm_next
            if step == 0:
                alpha = norm_next / energy
                direction = residual
            else:
                ratio = norm_next / norm_now
                alpha = norm_next / (energy - ratio * norm_next / alpha)
                direction = residual + ratio * direction
            norm_now = norm_next
            solution = solution + alpha * direction
            if step + 1 < STEPS:
                image = collect(seen) + penalty * residual
                along = image if step == 0 else image + ratio * along
                residual = residual - alpha * along
        merged = solution + scaled_dual
        sparse = jnp.sign(merged) * jnp.maximum(jnp.abs(merged) - thresh, 0.0)
        scaled_dual = merged - sparse
        return solution, sparse, scaled_dual

    vector = P(None, ("col", "row"))
    return jax.shard_map(
        on_device,
        mesh=mesh,
        in_specs=(P("row", "col"), P(None, "row"), vector, vector, vector, P()),
        out_specs=(vector, vector, vector),
        check_vma=False,
    )
```

```python
import functools

import jax
import jax.numpy as jnp
from jax import lax
from jax.experimental import pallas as pl
from jax.experimental.pallas import tpu as pltpu
from jax.sharding import PartitionSpec as P

STEPS = 3
LANES = 128
MESH = pl.DeviceIdType.MESH

penalty = 0.5


def halves(values):
    high = lax.reduce_precision(values, 8, 7)
    return high.astype(jnp.bfloat16), (values - high).astype(jnp.bfloat16)


def product(values, high, low, dims):
    rows = values.shape[0]
    top, rest = halves(values)
    dot = functools.partial(
        lax.dot_general, dimension_numbers=(dims, ((), ())), preferred_element_type=jnp.float32
    )
    both = dot(jnp.concatenate([top, rest], axis=0), high)
    return both[:rows] + (both[rows:] + dot(top, low))


def row_sums(values):
    return jnp.sum(values, axis=1, keepdims=True)


def spread_kernel(
    nr, nc, vector_ref, high_ref, low_ref, out_ref, total_ref,
    held, parts, acc, mine, land, stat, stat_land,
    load_high, load_low, line_send, line_recv, pair_send, pair_recv,
    col_send, col_recv, row_send, row_recv,
):
    row, col = lax.axis_index("row"), lax.axis_index("col")
    line = nr // 2
    z, core = row // 2, row % 2
    other = 1 - core
    depth, (rows, width) = high_ref.shape[0], vector_ref.shape
    hops = 2 * (line - 1)

    def load(slot):
        columns = pl.ds(pl.multiple_of(slot * width, LANES), width)
        return (
            pltpu.make_async_copy(
                high_ref.at[:, columns], parts.at[slot, pl.ds(0, depth)], load_high.at[slot]
            ),
            pltpu.make_async_copy(
                low_ref.at[:, columns], parts.at[slot, pl.ds(depth, depth)], load_low.at[slot]
            ),
        )

    def start_load(slot):
        for copy in load(slot):
            copy.start()

    def hop(i):
        sign = 1 - 2 * (i % 2)
        return sign, z - sign * (1 + i // 2)

    def inside(place):
        return jnp.logical_and(place >= 0, place < line)

    def along(source, slot, i, sign):
        return pltpu.make_async_remote_copy(
            src_ref=source,
            dst_ref=held.at[slot],
            send_sem=line_send.at[i],
            recv_sem=line_recv.at[i],
            device_id={"row": (z + sign) * 2 + core},
            device_id_type=MESH,
        )

    def across(source, slot, i):
        return pltpu.make_async_remote_copy(
            src_ref=source,
            dst_ref=held.at[slot],
            send_sem=pair_send.at[i],
            recv_sem=pair_recv.at[i],
            device_id={"row": z * 2 + other},
            device_id_type=MESH,
        )

    start_load(row)
    start_load(z * 2 + other)

    @pl.loop(0, hops)
    def _(i):
        _, origin = hop(i)

        @pl.when(inside(origin))
        def _():
            start_load(origin * 2 + core)
            start_load(origin * 2 + other)

    barrier = pltpu.get_barrier_semaphore()
    for s in range(1, nc):
        pl.semaphore_signal(
            barrier, inc=1, device_id={"col": lax.rem(col + s, nc)}, device_id_type=MESH
        )
    for s in range(1, nr):
        pl.semaphore_signal(
            barrier, inc=1, device_id={"row": lax.rem(row + s, nr)}, device_id_type=MESH
        )
    pl.semaphore_wait(barrier, nc + nr - 2)

    for i, sign in enumerate((1, -1)):

        @pl.when(inside(z + sign))
        def _():
            along(vector_ref, row, i, sign).start()

    across(vector_ref, row, hops).start()
    held[row] = vector_ref[...]
    acc[...] = jnp.zeros_like(acc)

    def multiply(slot):
        for copy in load(slot):
            copy.wait()
        values = held[slot]
        top = values.astype(jnp.bfloat16)
        rest = (values - top.astype(jnp.float32)).astype(jnp.bfloat16)
        acc[...] += lax.dot_general(
            parts[slot],
            jnp.concatenate([top, rest], axis=0),
            (((1,), (1,)), ((), ())),
            preferred_element_type=jnp.float32,
        )

    multiply(row)
    across(vector_ref, z * 2 + other, hops).wait_recv()
    multiply(z * 2 + other)

    @pl.loop(0, hops)
    def _(i):
        sign, origin = hop(i)
        slot = origin * 2 + core

        @pl.when(inside(origin))
        def _():
            along(held.at[slot], slot, i, sign).wait_recv()

            @pl.when(jnp.logical_and(inside(z + sign), i + 2 < hops))
            def _():
                along(held.at[slot], slot, i + 2, sign).start()

            across(held.at[slot], slot, i).start()
            multiply(slot)
            far = origin * 2 + other
            across(held.at[far], far, i).wait_recv()
            multiply(far)

    both = acc[pl.ds(0, depth)] + acc[pl.ds(depth, depth)]
    both = jnp.transpose(both)
    values = vector_ref[...]
    norm = jnp.sum(values * values, axis=1, keepdims=True)
    mine[:, :depth] = both[:rows] + both[rows:]
    mine[:, depth:] = jnp.broadcast_to(norm, (rows, LANES))

    @pl.loop(0, hops)
    def _(i):
        sign, origin = hop(i)

        @pl.when(jnp.logical_and(inside(z + sign), inside(origin + sign)))
        def _():
            along(vector_ref, row, i, sign).wait_send()

        @pl.when(inside(origin))
        def _():
            across(vector_ref, row, i).wait_send()

    across(vector_ref, row, hops).wait_send()

    copies = []
    for s in range(1, nc):
        copy = pltpu.make_async_remote_copy(
            src_ref=mine,
            dst_ref=land.at[col],
            send_sem=col_send.at[s - 1],
            recv_sem=col_recv.at[s - 1],
            device_id={"col": lax.rem(col + s, nc)},
            device_id_type=MESH,
        )
        copy.start()
        copies.append(copy)
    land[col] = mine[...]
    for copy in copies:
        copy.wait_recv()
    summed = land[0]
    for s in range(1, nc):
        summed = summed + land[s]
    product_values = summed[:, :depth]
    out_ref[...] = product_values
    square = jnp.sum(product_values * product_values, axis=1, keepdims=True)
    lane = lax.broadcasted_iota(jnp.int32, stat.shape, 1)
    told = jnp.where(lane < LANES // 2, summed[:, depth:], square)
    stat[...] = told
    stat_land[row] = told
    for s in range(1, nr):
        copy = pltpu.make_async_remote_copy(
            src_ref=stat,
            dst_ref=stat_land.at[row],
            send_sem=row_send.at[s - 1],
            recv_sem=row_recv.at[s - 1],
            device_id={"row": lax.rem(row + s, nr)},
            device_id_type=MESH,
        )
        copy.start()
        copies.append(copy)
    for copy in copies[nc - 1:]:
        copy.wait_recv()
    total = stat_land[0]
    for s in range(1, nr):
        total = total + stat_land[s]
    total_ref[...] = total
    for copy in copies:
        copy.wait_send()


def solution(mesh):
    nr, nc = mesh.shape["row"], mesh.shape["col"]

    def spread_call(vector, high, low):
        rows, width = vector.shape
        depth = high.shape[0]
        hops = nr - 2
        vmem = pl.BlockSpec(memory_space=pltpu.VMEM)
        hbm = pl.BlockSpec(memory_space=pl.ANY)
        values, total = pl.pallas_call(
            functools.partial(spread_kernel, nr, nc),
            out_shape=(
                jax.ShapeDtypeStruct((rows, depth), jnp.float32),
                jax.ShapeDtypeStruct((rows, LANES), jnp.float32),
            ),
            in_specs=[vmem, hbm, hbm],
            out_specs=(vmem, vmem),
            scratch_shapes=[
                pltpu.VMEM((nr, rows, width), jnp.float32),
                pltpu.VMEM((nr, 2 * depth, width), jnp.bfloat16),
                pltpu.VMEM((2 * depth, 2 * rows), jnp.float32),
                pltpu.VMEM((rows, depth + LANES), jnp.float32),
                pltpu.VMEM((nc, rows, depth + LANES), jnp.float32),
                pltpu.VMEM((rows, LANES), jnp.float32),
                pltpu.VMEM((nr, rows, LANES), jnp.float32),
                pltpu.SemaphoreType.DMA((nr,)),
                pltpu.SemaphoreType.DMA((nr,)),
                pltpu.SemaphoreType.DMA((hops,)),
                pltpu.SemaphoreType.DMA((hops,)),
                pltpu.SemaphoreType.DMA((hops + 1,)),
                pltpu.SemaphoreType.DMA((hops + 1,)),
                pltpu.SemaphoreType.DMA((nc - 1,)),
                pltpu.SemaphoreType.DMA((nc - 1,)),
                pltpu.SemaphoreType.DMA((nr - 1,)),
                pltpu.SemaphoreType.DMA((nr - 1,)),
            ],
            compiler_params=pltpu.CompilerParams(
                collective_id=0, has_side_effects=True, vmem_limit_bytes=48 * 1024 * 1024
            ),
        )(vector, high, low)
        return values, total[:, :1], total[:, LANES - 1:]

    def on_device(design, targets, warm_solution, warm_sparse, warm_dual, sparsity):
        high, low = halves(design)

        def spread(vector):
            return spread_call(vector, high, low)

        def collect(values):
            part = product(values, high, low, ((1,), (0,)))
            return lax.psum_scatter(part, "row", scatter_dimension=1, tiled=True)

        solution, sparse, scaled_dual = warm_solution, warm_sparse, warm_dual
        thresh = (sparsity / penalty)[:, None]
        seen, _, _ = spread(solution)
        residual = collect(targets - seen) + penalty * ((sparse - scaled_dual) - solution)
        direction = along = norm_now = alpha = None
        for step in range(STEPS):
            seen, norm_next, square = spread(residual)
            energy = square + penalty * norm_next
            if step == 0:
                alpha = norm_next / energy
                direction = residual
            else:
                ratio = norm_next / norm_now
                alpha = norm_next / (energy - ratio * norm_next / alpha)
                direction = residual + ratio * direction
            norm_now = norm_next
            solution = solution + alpha * direction
            if step + 1 < STEPS:
                image = collect(seen) + penalty * residual
                along = image if step == 0 else image + ratio * along
                residual = residual - alpha * along
        merged = solution + scaled_dual
        sparse = jnp.sign(merged) * jnp.maximum(jnp.abs(merged) - thresh, 0.0)
        scaled_dual = merged - sparse
        return solution, sparse, scaled_dual

    vector = P(None, ("col", "row"))
    return jax.shard_map(
        on_device,
        mesh=mesh,
        in_specs=(P("row", "col"), P(None, "row"), vector, vector, vector, P()),
        out_specs=(vector, vector, vector),
        check_vma=False,
    )
```
